32 devices in a mesh: dp: 4 (over y, x), expert: 8 (over z, core).
Axes of the slice: x: 2, y: 2, z: 4, core: 2. Of those that a mesh axis runs over, the one named last changes fastest.
Arguments:
- tokens: bfloat16 [4096, 2048], P(('dp', 'expert')), may hold values from -6 to 6
- expert_ids: int32 [4096, 2], P(('dp', 'expert')), may hold values from 0 to 7, all different within a row; in each aligned block of 128 rows (0 to 127, 128 to 255, ...) at most 40 rows name the same one
- gate_units: int32 [4096, 2], P(('dp', 'expert')), may hold values from 64 to 1023
- capacity: int32 [8], replicated, may hold values from 512 to 1535
- w_gate: bfloat16 [8, 2048, 1408], P('expert', None, 'dp'), may hold values from -0.125 to 0.125
- w_up: bfloat16 [8, 2048, 1408], P('expert', None, 'dp'), may hold values from -0.125 to 0.125
- w_down: bfloat16 [8, 2048, 1408], P('expert', None, 'dp'), may hold values from -0.15625 to 0.15625
Outputs:
- mixed: bfloat16 [4096, 2048], P(('dp', 'expert'))
The draws below stay inside these ranges and needn't reach their ends.
Inputs may be any that keep to these rules, and one draw needn't show every extreme that they name: `expert_ids`: each row names two different experts; of one device's 128 rows (aligned blocks) no expert is named more than 40 times.
All inputs are finite; a program needn't handle non-finite values.
Results may differ from the reference program's by a relative error of at most 0.0057.
Values may be sent and summed in bfloat16 or wider, within the bound.
No kernel may reach another device: no remote copies, remote signals or barrier semaphores. Data moves between devices by JAX's collectives and lax.ppermute only.
A program may use at most 128 MiB of HBM per device.

```python
import math
import jax
import jax.numpy as jnp
import numpy as np
from jax import lax

D = 2048
FF = 1408
TOK_DEV = 128
EXPERTS = 8
TOKENS = 4096
MOST = 40
CAP_HI = 1536


def touch_ends(values, key, low, top_value):
    place = [jax.random.randint(jax.random.fold_in(key, axis), (), 0, length) for axis, length in enumerate(values.shape)]
    main_axis = values.shape.index(max(values.shape))
    neighbour = place[:main_axis] + [(place[main_axis] + 1) % values.shape[main_axis]] + place[main_axis + 1:]
    return values.at[tuple(place)].set(low).at[tuple(neighbour)].set(top_value)


def level_of(key, shape, split, smallest, top_value):
    loudness, own = 1.0, jax.random.fold_in(key, 6)
    for position, shards_of in split:
        heights = jnp.exp(jax.random.uniform(jax.random.fold_in(own, position), (shards_of,), jnp.float32, smallest / len(split), top_value / len(split)))
        loudness = loudness * jnp.repeat(heights, shape[position] // shards_of).reshape([-1 if axis == position else 1 for axis in range(len(shape))])
    return loudness


def routed_block(key, own, number, rows, number_of, top, limit, lean):
    sequence = jax.random.permutation(key, number_of)
    packed, ordinary = load_shares(number_of, rows * top, limit, lean, True), load_shares(number_of, rows * top, limit, lean, False)
    places = jnp.arange(number_of)

    def named(lengths, turn):
        used = int((lengths > 0).sum())
        fixed = max(1, used // 4)
        shifted = fixed + (places - fixed + turn * (used - fixed)) % max(1, number_of - fixed)
        return jnp.zeros((number_of,), jnp.int32).at[sequence[jnp.where(places < fixed, places, shifted)]].set(jnp.asarray(lengths, jnp.int32))

    lengths = jnp.where(number % 4 == 0, named(packed, number // 4), named(ordinary, number - number // 4 - 1))
    mixed = jax.random.permutation(jax.random.fold_in(own, 3), number_of)
    giver, taker = mixed[0:number_of // 2 * 2:2], mixed[1:number_of // 2 * 2:2]
    room = jnp.minimum(lengths[giver] - 1, limit - lengths[taker]) // 2
    room = jnp.where((giver == sequence[0]) | (taker == sequence[0]) | (lengths[taker] == 0), 0, jnp.maximum(room, 0))
    shifted = jax.random.randint(jax.random.fold_in(own, 4), (number_of // 2,), 0, 1 << 20) % (room + 1)
    lengths = lengths.at[giver].add(-shifted).at[taker].add(shifted)
    items = jnp.searchsorted(jnp.cumsum(lengths), jnp.arange(rows * top), side="right").astype(jnp.int32)
    listing = items.reshape(top, rows).T
    listing = listing[jax.random.permutation(jax.random.fold_in(own, 1), rows)]
    turn = jax.random.randint(jax.random.fold_in(own, 2), (rows, 1), 0, top)
    return jnp.take_along_axis(listing, (jnp.arange(top)[None, :] + turn) % top, axis=1)


def load_shares(amount, total, limit, skew, full):
    weights = [(1 << 20) // math.isqrt(standing ** skew) + 1 for standing in range(1, amount + 1)]
    largest = limit if full else min(limit, max(-(-total // amount), total * weights[0] // sum(weights)))
    least = 1 if total - largest >= amount - 1 else 0
    counts, spare = [largest] + [least] * (amount - 1), total - largest - least * (amount - 1)
    while spare > 0:
        movable = [i for i in range(1, amount) if counts[i] < largest] or [i for i in range(1, amount) if counts[i] < limit]
        whole, left = sum([weights[i] for i in movable]), spare
        for i in movable:
            extra = min(limit - counts[i], max(1, left * weights[i] // whole), spare)
            counts[i] = counts[i] + extra
            spare = spare - extra
    return np.array(counts)


def noise(key, dims, width, limit, shards=(), kind=jnp.bfloat16):
    loudness = level_of(key, dims, shards, -0.22, 0.18) if shards else 1.0
    values = jax.random.normal(key, dims, jnp.float32) * width * loudness
    return jnp.minimum(jnp.maximum(values, -limit), limit).astype(kind)


def setup_inputs(seed: int = 0) -> dict:
    arg_keys = jax.random.split(jax.random.key(seed), 8)
    tokens = noise(arg_keys[0], (TOKENS, D), 1.0, 6.0, ((0, 32),))
    expert_ids_keys = jax.random.split(jax.random.fold_in(arg_keys[1], 1), TOKENS // TOK_DEV)
    expert_ids_turns = jax.random.permutation(jax.random.fold_in(arg_keys[1], 3), TOKENS // TOK_DEV)
    expert_ids = jax.vmap(lambda own, number: routed_block(jax.random.fold_in(arg_keys[1], 2), own, number, TOK_DEV, EXPERTS, 2, MOST, 1))(expert_ids_keys, expert_ids_turns).reshape((TOKENS, 2))
    gate_units = touch_ends(jax.random.randint(arg_keys[2], (TOKENS, 2), 64, 1024), jax.random.fold_in(arg_keys[2], 1), 64, 1023).astype(jnp.int32)
    capacity = touch_ends(jax.random.randint(arg_keys[3], (EXPERTS,), TOKENS // EXPERTS, CAP_HI), jax.random.fold_in(arg_keys[3], 1), TOKENS // EXPERTS, CAP_HI - 1).astype(jnp.int32)
    w_gate = noise(arg_keys[4], (EXPERTS, D, FF), D ** -0.5, 0.125, ((0, 8), (2, 4)))
    w_up = noise(arg_keys[5], (EXPERTS, D, FF), D ** -0.5, 0.125, ((0, 8), (2, 4)))
    w_down = noise(arg_keys[6], (EXPERTS, D, FF), FF ** -0.5, 0.15625, ((0, 8), (2, 4)))
    return {"tokens": tokens, "expert_ids": expert_ids, "gate_units": gate_units, "capacity": capacity, "w_gate": w_gate, "w_up": w_up, "w_down": w_down}


def expert_rows(rows, gate_w, up_w, down_w):
    gate = jnp.dot(rows, gate_w, preferred_element_type=jnp.float32)
    up = jnp.dot(rows, up_w, preferred_element_type=jnp.float32)
    hidden = (jax.nn.silu(gate) * up).astype(jnp.bfloat16)
    return lax.dot_general(hidden, down_w, (((1,), (1,)), ((), ())), preferred_element_type=jnp.float32)


def reference(tokens, expert_ids, gate_units, capacity, w_gate, w_up, w_down):
    flat = expert_ids.reshape(-1).astype(jnp.int32)
    onehot = (flat[:, None] == jnp.arange(EXPERTS, dtype=jnp.int32)[None, :]).astype(jnp.int32)
    slot = jnp.sum((jnp.cumsum(onehot, axis=0) - onehot) * onehot, axis=1).astype(jnp.int32)
    kept = slot < capacity[flat]
    weight = jnp.where(kept, gate_units.reshape(-1).astype(jnp.float32) / 1024.0, jnp.float32(0.0))
    token_of = (jnp.arange(2 * TOKENS, dtype=jnp.int32) // 2).astype(jnp.int32)

    def per_expert(carry, index):
        target = jnp.where((flat == index) & kept, slot, CAP_HI).astype(jnp.int32)
        rows_index = jnp.zeros((CAP_HI,), jnp.int32).at[target].set(token_of, mode="drop")
        scales = jnp.zeros((CAP_HI,), jnp.float32).at[target].set(weight, mode="drop")
        result = expert_rows(tokens[rows_index], w_gate[index], w_up[index], w_down[index])
        result = result.astype(jnp.bfloat16).astype(jnp.float32)
        carry = carry.at[rows_index].add(result * scales[:, None])
        return carry, None

    total, _ = lax.scan(per_expert, jnp.zeros((TOKENS, D), jnp.float32), jnp.arange(EXPERTS, dtype=jnp.int32))
    return total.astype(jnp.bfloat16)
```

```python
import jax
import jax.numpy as jnp
from jax import lax
from jax.sharding import PartitionSpec as P

BF16 = jnp.bfloat16
F32 = jnp.float32
AXES = ("dp", "expert")


def far_first(n):
    return sorted(range(1, n), key=lambda k: (-(k // 2), k))


def pair_permute(values, n_dp, n_exp, weights_side):
    pairs = []
    for d in range(n_dp):
        for e in range(n_exp):
            high = (e % 2 == 0) == weights_side
            partner = d ^ (n_dp // 2) if high else d ^ 1
            pairs.append((d * n_exp + e, partner * n_exp + e))
    return lax.ppermute(values, AXES, pairs)


def few(n):
    return n - 1 <= 16


def expert_exchange(blocks):
    n = lax.axis_size("expert")
    if not few(n):
        place = jnp.arange(n, dtype=jnp.int32) ^ lax.axis_index("expert")
        there = lax.all_to_all(jnp.stack(blocks)[place], "expert", 0, 0, tiled=True)[place]
        return [there[k] for k in range(n)]
    out = [blocks[0]] + [None] * (n - 1)
    for k in far_first(n):
        out[k] = lax.ppermute(blocks[k], "expert", [(i, i ^ k) for i in range(n)])
    return out


def earlier_counts(counts, late):
    n = lax.axis_size("dp") * lax.axis_size("expert")
    me = lax.axis_index(AXES)
    total, before = counts, jnp.zeros_like(counts)
    step = 1
    while step < n:
        if step == lax.axis_size("expert"):
            total, _ = lax.optimization_barrier((total, late))
        other = lax.ppermute(total, AXES, [(i, i ^ step) for i in range(n)])
        before = before + jnp.where((me & step) != 0, other, 0)
        total = total + other
        step *= 2
    return before


def dot(a, b):
    return jnp.dot(a, b, preferred_element_type=F32)


def hidden_of(rows, gate_w, up_w):
    return (jax.nn.silu(dot(rows, gate_w)) * dot(rows, up_w)).astype(BF16)


def down(hidden, w):
    return lax.dot_general(hidden, w, (((1,), (1,)), ((), ())), preferred_element_type=F32)


def layer(tokens, expert_ids, gate_units, capacity, w_gate, w_up, w_down):
    n_dp, n_exp = lax.axis_size("dp"), lax.axis_size("expert")
    tok_rows, width = tokens.shape
    n_experts = capacity.shape[0]
    most = max(2, 5 * tok_rows // (2 * n_experts))
    me = lax.axis_index("expert")
    wg, wu, wd = w_gate[0], w_up[0], w_down[0]
    wg2 = pair_permute(wg, n_dp, n_exp, True)
    wu2 = pair_permute(wu, n_dp, n_exp, True)
    wd2 = pair_permute(wd, n_dp, n_exp, True)

    places = jnp.arange(n_experts, dtype=jnp.int32)
    away = expert_ids ^ me
    named = away[:, :, None] == places[None, None, :]
    once = jnp.any(named, axis=1)
    t = jnp.arange(tok_rows, dtype=jnp.int32)
    lower = (t[:, None] > t[None, :]).astype(BF16)
    rank = dot(lower, once.astype(BF16)).astype(jnp.int32)
    slot = jnp.where(once, rank, most).T
    chosen = slot[:, None, :] == jnp.arange(most, dtype=jnp.int32)[None, :, None]
    chosen = chosen.reshape(n_experts * most, tok_rows)
    outgoing = dot(chosen.astype(BF16), tokens).astype(BF16).reshape(n_experts, most, width)

    arrived = jnp.concatenate(expert_exchange([outgoing[k] for k in range(n_experts)]), axis=0)
    theirs = pair_permute(arrived, n_dp, n_exp, False)

    part_theirs = down(hidden_of(theirs, wg, wu), wd) + down(hidden_of(theirs, wg2, wu2), wd2)
    returned = pair_permute(part_theirs.astype(BF16), n_dp, n_exp, False)
    part_own = down(hidden_of(arrived, wg, wu), wd) + down(hidden_of(arrived, wg2, wu2), wd2)
    answer = (part_own + returned.astype(F32)).astype(BF16).reshape(n_experts, most, width)
    back = jnp.concatenate(expert_exchange([answer[k] for k in range(n_experts)]), axis=0)

    counts = jnp.sum((expert_ids[:, :, None] == places).astype(jnp.int32), axis=(0, 1))
    counts, _ = lax.optimization_barrier((counts, arrived[0, 0]))
    room = capacity - earlier_counts(counts, answer[0, 0, 0])
    room_of = jnp.sum(jnp.where(expert_ids[:, :, None] == places, room, 0), axis=2)
    rank_of = jnp.sum(jnp.where(named, rank[:, None, :], 0), axis=2)
    units = jnp.where(rank_of < room_of, gate_units, 0)
    unit_at = jnp.sum(jnp.where(named, units[:, :, None], 0), axis=1)
    high = (unit_at // 8 * 8).astype(F32) / 1024.0
    low = (unit_at % 8).astype(F32) / 1024.0

    picks = chosen.reshape(n_experts, most, tok_rows)
    high_at = jnp.where(picks, high.T[:, None, :], 0.0).astype(BF16).reshape(n_experts * most, tok_rows)
    low_at = jnp.where(picks, low.T[:, None, :], 0.0).astype(BF16).reshape(n_experts * most, tok_rows)
    across = (((0,), (0,)), ((), ()))
    mixed = lax.dot_general(high_at, back, across, preferred_element_type=F32)
    mixed = mixed + lax.dot_general(low_at, back, across, preferred_element_type=F32)
    return mixed.astype(BF16)


def solution(mesh):
    return jax.shard_map(
        layer,
        mesh=mesh,
        in_specs=(
            P(AXES, None),
            P(AXES, None),
            P(AXES, None),
            P(),
            P("expert", None, "dp"),
            P("expert", None, "dp"),
            P("expert", None, "dp"),
        ),
        out_specs=P(AXES, None),
        check_vma=False,
    )
```

```python
import jax
import jax.numpy as jnp
from jax import lax
from jax.experimental import pallas as pl
from jax.experimental.pallas import tpu as pltpu
from jax.sharding import PartitionSpec as P

BF16 = jnp.bfloat16
F32 = jnp.float32
AXES = ("dp", "expert")
VMEM_LIMIT = 8 << 20
BOTH_LAST = (((1,), (1,)), ((), ()))
BOTH_FIRST = (((0,), (0,)), ((), ()))


def few(n):
    return n - 1 <= 16


def near_far(n):
    return list(range(n // 2)), list(range(n // 2, n))


def pair_permute(values, n_dp, n_exp, weights_side):
    pairs = []
    for d in range(n_dp):
        for e in range(n_exp):
            high = (e % 2 == 0) == weights_side
            partner = d ^ (n_dp // 2) if high else d ^ 1
            pairs.append((d * n_exp + e, partner * n_exp + e))
    return lax.ppermute(values, AXES, pairs)


def expert_exchange(blocks):
    n = lax.axis_size("expert")
    if not few(n):
        place = jnp.arange(n, dtype=jnp.int32) ^ lax.axis_index("expert")
        there = lax.all_to_all(jnp.stack(blocks)[place], "expert", 0, 0, tiled=True)[place]
        return [there[k] for k in range(n)]
    out = [blocks[0]] + [None] * (n - 1)
    for k in range(1, n):
        out[k] = lax.ppermute(blocks[k], "expert", [(i, i ^ k) for i in range(n)])
    return out


def earlier_counts(counts, late):
    n = lax.axis_size("dp") * lax.axis_size("expert")
    me = lax.axis_index(AXES)
    total, before = counts, jnp.zeros_like(counts)
    step = 1
    while step < n:
        if step == lax.axis_size("expert"):
            total, _ = lax.optimization_barrier((total, late))
        other = lax.ppermute(total, AXES, [(i, i ^ step) for i in range(n)])
        before = before + jnp.where((me & step) != 0, other, 0)
        total = total + other
        step *= 2
    return before


def dot(a, b):
    return jnp.dot(a, b, preferred_element_type=F32)


def kernel_call(body, shapes, operands, flops):
    spec = pl.BlockSpec(memory_space=pltpu.VMEM)
    single = not isinstance(shapes, (list, tuple))
    moved = sum(x.size * x.dtype.itemsize for x in operands)
    return pl.pallas_call(
        body,
        out_shape=shapes if single else tuple(shapes),
        in_specs=[spec] * len(operands),
        out_specs=spec if single else tuple([spec] * len(shapes)),
        compiler_params=pltpu.CompilerParams(vmem_limit_bytes=VMEM_LIMIT),
        cost_estimate=pl.CostEstimate(flops=flops, bytes_accessed=moved, transcendentals=0),
    )(*operands)


def join(blocks):
    if len(blocks) > 16:
        return jnp.concatenate(blocks, axis=0)
    rows, width = blocks[0].shape

    def body(*refs):
        for i, ref in enumerate(refs[:-1]):
            refs[-1][i * rows : (i + 1) * rows, :] = ref[...]

    shape = jax.ShapeDtypeStruct((rows * len(blocks), width), blocks[0].dtype)
    return kernel_call(body, shape, blocks, 0)


def hidden_of(rows, gate_t, up_t):
    def body(rows_ref, gate_ref, up_ref, out_ref):
        gate = lax.dot_general(rows_ref[...], gate_ref[...], BOTH_LAST, preferred_element_type=F32)
        up = lax.dot_general(rows_ref[...], up_ref[...], BOTH_LAST, preferred_element_type=F32)
        out_ref[...] = (gate / (1.0 + jnp.exp(-gate)) * up).astype(BF16)

    units = gate_t.shape[0]
    shape = jax.ShapeDtypeStruct((rows.shape[0], units), BF16)
    return kernel_call(body, shape, (rows, gate_t, up_t), 4 * rows.size * units)


def down(hidden, down_t, hidden2, down2_t, dtype):
    width = down_t.shape[1]
    step = min(width, 512)

    def body(h_ref, w_ref, h2_ref, w2_ref, out_ref):
        for at in range(0, width, step):
            part = dot(h_ref[...], w_ref[:, at : at + step]) + dot(h2_ref[...], w2_ref[:, at : at + step])
            out_ref[:, at : at + step] = part.astype(out_ref.dtype)

    shape = jax.ShapeDtypeStruct((hidden.shape[0], width), dtype)
    return kernel_call(body, shape, (hidden, down_t, hidden2, down2_t), 4 * hidden.size * width)


def add_and_split(own, returned, count):
    rows, width = own.shape[0] // count, own.shape[1]
    if count > 16:
        total = (own + returned.astype(F32)).astype(BF16).reshape(count, rows, width)
        return [total[k] for k in range(count)]

    def body(own_ref, returned_ref, *out_refs):
        for k, ref in enumerate(out_refs):
            part = slice(k * rows, (k + 1) * rows)
            ref[...] = (own_ref[part, :] + returned_ref[part, :].astype(F32)).astype(BF16)

    shapes = [jax.ShapeDtypeStruct((rows, width), BF16)] * count
    return list(kernel_call(body, shapes, (own, returned), own.size))


def layer(tokens, expert_ids, gate_units, capacity, w_gate, w_up, w_down):
    n_dp, n_exp = lax.axis_size("dp"), lax.axis_size("expert")
    tok_rows, width = tokens.shape
    n_experts = capacity.shape[0]
    most = max(2, 5 * tok_rows // (2 * n_experts))
    me = lax.axis_index("expert")
    near, far = near_far(n_experts)
    wg, wu, wd = w_gate[0].T, w_up[0].T, w_down[0].T
    wg2 = pair_permute(wg, n_dp, n_exp, True)
    wu2 = pair_permute(wu, n_dp, n_exp, True)
    wd2 = pair_permute(wd, n_dp, n_exp, True)

    places = jnp.arange(n_experts, dtype=jnp.int32)
    away = expert_ids ^ me
    named = away[:, :, None] == places[None, None, :]
    once = jnp.any(named, axis=1)
    t = jnp.arange(tok_rows, dtype=jnp.int32)
    lower = (t[:, None] > t[None, :]).astype(BF16)
    rank = dot(lower, once.astype(BF16)).astype(jnp.int32)
    slot = jnp.where(once, rank, most).T
    chosen = slot[:, None, :] == jnp.arange(most, dtype=jnp.int32)[None, :, None]
    chosen = chosen.reshape(n_experts * most, tok_rows)
    outgoing = dot(chosen.astype(BF16), tokens).astype(BF16).reshape(n_experts, most, width)

    arrived = expert_exchange([outgoing[k] for k in range(n_experts)])
    own_near = join([arrived[k] for k in near])
    theirs_near = pair_permute(own_near, n_dp, n_exp, False)
    own_far = join([arrived[k] for k in far])
    theirs_far = pair_permute(own_far, n_dp, n_exp, False)

    def hidden_pair(rows):
        return hidden_of(rows, wg, wu), hidden_of(rows, wg2, wu2)

    def partial(pair, dtype):
        return down(pair[0], wd, pair[1], wd2, dtype)

    h_own_near = hidden_pair(own_near)
    h_own_far = hidden_pair(own_far)
    h_near = hidden_pair(theirs_near)
    h_far = hidden_pair(theirs_far)
    back_far = pair_permute(partial(h_far, BF16), n_dp, n_exp, False)
    back_near = pair_permute(partial(h_near, BF16), n_dp, n_exp, False)
    own_far_part = partial(h_own_far, F32)
    own_near_part = partial(h_own_near, F32)
    answer_far = add_and_split(own_far_part, back_far, len(far))
    answer_near = add_and_split(own_near_part, back_near, len(near))
    back = expert_exchange(answer_near + answer_far)

    counts = jnp.sum((expert_ids[:, :, None] == places).astype(jnp.int32), axis=(0, 1))
    counts, _ = lax.optimization_barrier((counts, own_far[0, 0]))
    room = capacity - earlier_counts(counts, answer_far[0][0, 0])
    room_of = jnp.sum(jnp.where(expert_ids[:, :, None] == places, room, 0), axis=2)
    rank_of = jnp.sum(jnp.where(named, rank[:, None, :], 0), axis=2)
    units = jnp.where(rank_of < room_of, gate_units, 0)
    unit_at = jnp.sum(jnp.where(named, units[:, :, None], 0), axis=1)
    high = (unit_at // 8 * 8).astype(F32) / 1024.0
    low = (unit_at % 8).astype(F32) / 1024.0
    picks = chosen.reshape(n_experts, most, tok_rows)
    high_at = jnp.where(picks, high.T[:, None, :], 0.0).astype(BF16).reshape(n_experts * most, tok_rows)
    low_at = jnp.where(picks, low.T[:, None, :], 0.0).astype(BF16).reshape(n_experts * most, tok_rows)

    def mix(high_ref, low_ref, *refs):
        joined, out_ref = refs[-1], refs[-2]
        for k, ref in enumerate(refs[:-2]):
            joined[k * most : (k + 1) * most, :] = ref[...]
        mixed = lax.dot_general(high_ref[...], joined[...], BOTH_FIRST, preferred_element_type=F32)
        mixed += lax.dot_general(low_ref[...], joined[...], BOTH_FIRST, preferred_element_type=F32)
        out_ref[...] = mixed.astype(BF16)

    if not few(n_experts):
        back = [jnp.concatenate(back, axis=0)]
        most = most * n_experts
    spec = pl.BlockSpec(memory_space=pltpu.VMEM)
    return pl.pallas_call(
        mix,
        out_shape=jax.ShapeDtypeStruct((tok_rows, width), BF16),
        in_specs=[spec] * (2 + len(back)),
        out_specs=spec,
        scratch_shapes=[pltpu.VMEM((len(back) * most, width), BF16)],
        compiler_params=pltpu.CompilerParams(vmem_limit_bytes=VMEM_LIMIT),
        name="mix",
    )(high_at, low_at, *back)


def solution(mesh):
    return jax.shard_map(
        layer,
        mesh=mesh,
        in_specs=(
            P(AXES, None),
            P(AXES, None),
            P(AXES, None),
            P(),
            P("expert", None, "dp"),
            P("expert", None, "dp"),
            P("expert", None, "dp"),
        ),
        out_specs=P(AXES, None),
        check_vma=False,
    )
```

```python
import functools

import jax
import jax.numpy as jnp
from jax import lax
from jax.experimental import pallas as pl
from jax.experimental.pallas import tpu as pltpu
from jax.sharding import PartitionSpec as P

BF16 = jnp.bfloat16
F32 = jnp.float32
AXES = ("dp", "expert")
VMEM_LIMIT = 8 << 20
BOTH_LAST = (((1,), (1,)), ((), ()))
BOTH_FIRST = (((0,), (0,)), ((), ()))


def few(n):
    return n - 1 <= 16


def near_far(n):
    return list(range(n // 2)), list(range(n // 2, n))


def pair_permute(values, n_dp, n_exp, weights_side):
    pairs = []
    for d in range(n_dp):
        for e in range(n_exp):
            high = (e % 2 == 0) == weights_side
            partner = d ^ (n_dp // 2) if high else d ^ 1
            pairs.append((d * n_exp + e, partner * n_exp + e))
    return lax.ppermute(values, AXES, pairs)


def expert_exchange(blocks):
    n = lax.axis_size("expert")
    if not few(n):
        place = jnp.arange(n, dtype=jnp.int32) ^ lax.axis_index("expert")
        there = lax.all_to_all(jnp.stack(blocks)[place], "expert", 0, 0, tiled=True)[place]
        return [there[k] for k in range(n)]
    return expert_send(blocks, range(n))


def expert_send(blocks, places):
    n, out = lax.axis_size("expert"), []
    for k, block in zip(places, blocks):
        if k:
            block = lax.ppermute(block, "expert", [(i, i ^ k) for i in range(n)])
        out.append(block)
    return out


def exchanged_counts(counts, late):
    n = lax.axis_size("dp") * lax.axis_size("expert")
    total, others = counts, []
    step = 1
    while step < n:
        if step == lax.axis_size("expert"):
            total, _ = lax.optimization_barrier((total, late))
        others.append(lax.ppermute(total, AXES, [(i, i ^ step) for i in range(n)]))
        total = total + others[-1]
        step *= 2
    return others


def dot(a, b):
    return jnp.dot(a, b, preferred_element_type=F32)


def kernel_call(body, shapes, operands, flops):
    spec = pl.BlockSpec(memory_space=pltpu.VMEM)
    single = not isinstance(shapes, (list, tuple))
    moved = sum(x.size * x.dtype.itemsize for x in operands)
    return pl.pallas_call(
        body,
        out_shape=shapes if single else tuple(shapes),
        in_specs=[spec] * len(operands),
        out_specs=spec if single else tuple([spec] * len(shapes)),
        compiler_params=pltpu.CompilerParams(vmem_limit_bytes=VMEM_LIMIT),
        cost_estimate=pl.CostEstimate(flops=flops, bytes_accessed=moved, transcendentals=0),
    )(*operands)


def join(blocks):
    if len(blocks) > 16:
        return jnp.concatenate(blocks, axis=0)
    rows, width = blocks[0].shape

    def body(*refs):
        for i, ref in enumerate(refs[:-1]):
            refs[-1][i * rows : (i + 1) * rows, :] = ref[...]

    shape = jax.ShapeDtypeStruct((rows * len(blocks), width), blocks[0].dtype)
    return kernel_call(body, shape, blocks, 0)


def hidden_of(rows, gate_t, up_t):
    def body(rows_ref, gate_ref, up_ref, out_ref):
        gate = lax.dot_general(rows_ref[...], gate_ref[...], BOTH_LAST, preferred_element_type=F32)
        up = lax.dot_general(rows_ref[...], up_ref[...], BOTH_LAST, preferred_element_type=F32)
        out_ref[...] = (gate / (1.0 + jnp.exp(-gate)) * up).astype(BF16)

    units = gate_t.shape[0]
    shape = jax.ShapeDtypeStruct((rows.shape[0], units), BF16)
    return kernel_call(body, shape, (rows, gate_t, up_t), 4 * rows.size * units)


def down(hidden, down_t, hidden2, down2_t, dtype, start=0):
    width = sum(piece.shape[1] for piece in down2_t)
    step = min(down2_t[0].shape[1], 512)

    def body(h_ref, w_ref, h2_ref, *refs):
        at = 0
        for ref in refs[:-1]:
            for here in range(0, ref.shape[1], step):
                columns = slice(start + at, start + at + step)
                part = dot(h_ref[...], w_ref[:, columns]) + dot(h2_ref[...], ref[:, here : here + step])
                refs[-1][:, at : at + step] = part.astype(dtype)
                at += step

    shape = jax.ShapeDtypeStruct((hidden.shape[0], width), dtype)
    return kernel_call(body, shape, (hidden, down_t, hidden2, *down2_t), 4 * hidden.size * width)


def add_and_split(own, returned, count):
    rows, width = own.shape[0] // count, own.shape[1]
    if count > 16:
        total = (own + returned.astype(F32)).astype(BF16).reshape(count, rows, width)
        return [total[k] for k in range(count)]

    def body(own_ref, returned_ref, *out_refs):
        for k, ref in enumerate(out_refs):
            part = slice(k * rows, (k + 1) * rows)
            ref[...] = (own_ref[part, :] + returned_ref[part, :].astype(F32)).astype(BF16)

    shapes = [jax.ShapeDtypeStruct((rows, width), BF16)] * count
    return list(kernel_call(body, shapes, (own, returned), own.size))


def named_places(ids, me, n):
    rows = ids.shape[1]
    place = lax.broadcasted_iota(jnp.int32, (n, rows), 0)
    named = [(ids[k : k + 1, :] ^ me) == place for k in range(ids.shape[0])]
    once = functools.reduce(jnp.logical_or, named)
    first = lax.broadcasted_iota(jnp.int32, (rows, rows), 0)
    second = lax.broadcasted_iota(jnp.int32, (rows, rows), 1)
    earlier = dot(ones_at(once), ones_at(first < second))
    return named, once, earlier


def ones_at(mask):
    return jnp.where(mask, 1.0, 0.0).astype(BF16)


def dispatch(tokens, ids, here, n, most):
    tok_rows, width = tokens.shape

    def body(tokens_ref, ids_ref, here_ref, counts_ref, *out_refs):
        me = here_ref[0, 0] % n
        _, once, earlier = named_places(ids_ref[...], me, n)
        _, absolute, _ = named_places(ids_ref[...], 0, n)
        ones = jnp.ones((1, tok_rows), BF16)
        counts = lax.dot_general(ones, ones_at(absolute), BOTH_LAST, preferred_element_type=F32)
        counts_ref[...] = counts.astype(jnp.int32)
        slot = jnp.where(once, earlier, -1.0)
        row = lax.broadcasted_iota(jnp.int32, (most, tok_rows), 0).astype(F32)
        for k in range(n):
            picked = dot(ones_at(row == slot[k : k + 1, :]), tokens_ref[...]).astype(BF16)
            if few(n):
                out_refs[k][...] = picked
            else:
                out_refs[0][k] = picked

    shapes = [jax.ShapeDtypeStruct((1, n), jnp.int32)]
    if few(n):
        shapes += [jax.ShapeDtypeStruct((most, width), BF16)] * n
    else:
        shapes += [jax.ShapeDtypeStruct((n, most, width), BF16)]
    memory = [pltpu.VMEM, pltpu.VMEM, pltpu.SMEM]
    call = pl.pallas_call(
        body,
        out_shape=tuple(shapes),
        in_specs=[pl.BlockSpec(memory_space=m) for m in memory],
        out_specs=tuple(pl.BlockSpec(memory_space=pltpu.VMEM) for _ in shapes),
        compiler_params=pltpu.CompilerParams(vmem_limit_bytes=VMEM_LIMIT),
        name="dispatch",
    )
    counts, *blocks = call(tokens, ids, here)
    return [blocks[0][k] for k in range(n)] if len(blocks) < n else blocks, counts


def mix(ids, units, capacity, others, here, back, corners, most):
    n, tok_rows, width = capacity.shape[1], ids.shape[1], sum(b.shape[0] * b.shape[1] for b in back)
    width = width // (n * most)

    def body(here_ref, ids_ref, units_ref, capacity_ref, *refs):
        other_refs, back_refs = refs[: len(others)], refs[len(others) : -2]
        out_ref, joined = refs[-2:]
        me = here_ref[0, 0]
        room = capacity_ref[...]
        for i, ref in enumerate(other_refs):
            room = room - ref[...] * ((me >> i) & 1)
        place = lax.broadcasted_iota(jnp.int32, (n, n), 0)
        expert = lax.broadcasted_iota(jnp.int32, (n, n), 1)
        room = jnp.sum(jnp.where(place ^ (me % n) == expert, room, 0).astype(F32), axis=1, keepdims=True)
        named, once, earlier = named_places(ids_ref[...], me % n, n)
        unit = sum(jnp.where(named[k], units_ref[k : k + 1, :], 0) for k in range(len(named)))
        unit = jnp.where(earlier < room, unit, 0)
        high = ((unit >> 3) << 3).astype(F32) * (1.0 / 1024.0)
        low = (unit & 7).astype(F32) * (1.0 / 1024.0)
        slot = jnp.where(once, earlier, -1.0)
        row = lax.broadcasted_iota(jnp.int32, (most, tok_rows), 0).astype(F32)

        def spread(values):
            parts = [jnp.where(row == slot[k : k + 1, :], values[k : k + 1, :], 0.0) for k in range(n)]
            return jnp.concatenate(parts, axis=0).astype(BF16)

        for at, ref in zip(corners, back_refs):
            joined[at[0] : at[0] + ref.shape[0], at[1] : at[1] + ref.shape[1]] = ref[...]
        mixed = lax.dot_general(spread(high), joined[...], BOTH_FIRST, preferred_element_type=F32)
        mixed += lax.dot_general(spread(low), joined[...], BOTH_FIRST, preferred_element_type=F32)
        out_ref[...] = mixed.astype(BF16)

    operands = (here, ids, units, capacity, *others, *back)
    memory = [pltpu.SMEM] + [pltpu.VMEM] * (len(operands) - 1)
    return pl.pallas_call(
        body,
        out_shape=jax.ShapeDtypeStruct((tok_rows, width), BF16),
        in_specs=[pl.BlockSpec(memory_space=m) for m in memory],
        out_specs=pl.BlockSpec(memory_space=pltpu.VMEM),
        scratch_shapes=[pltpu.VMEM((n * most, width), BF16)],
        compiler_params=pltpu.CompilerParams(vmem_limit_bytes=VMEM_LIMIT),
        name="mix",
    )(*operands)


def layer(tokens, expert_ids, gate_units, capacity, w_gate, w_up, w_down):
    n_dp, n_exp = lax.axis_size("dp"), lax.axis_size("expert")
    tok_rows, width = tokens.shape
    n_experts = capacity.shape[0]
    most = max(2, 5 * tok_rows // (2 * n_experts))
    here = jnp.full((1, 1), lax.axis_index(AXES), jnp.int32)
    near, far = near_far(n_experts)
    wg, wu, wd = w_gate[0].T, w_up[0].T, w_down[0].T
    here, wg, wu, wd = lax.optimization_barrier((here, wg, wu, wd))
    wg2 = pair_permute(wg, n_dp, n_exp, True)
    wu2 = pair_permute(wu, n_dp, n_exp, True)
    half = width // 2
    wd2_a = pair_permute(wd[:, :half], n_dp, n_exp, True)
    wd2_b = pair_permute(wd[:, half:], n_dp, n_exp, True)

    ids = expert_ids.T
    blocks, counts = dispatch(tokens, ids, here, n_experts, most)
    arrived = expert_exchange(blocks)
    own_near = join([arrived[k] for k in near])
    theirs_near = pair_permute(own_near, n_dp, n_exp, False)
    own_far = join([arrived[k] for k in far])
    theirs_far = pair_permute(own_far, n_dp, n_exp, False)

    def hidden_pair(rows):
        return hidden_of(rows, wg, wu), hidden_of(rows, wg2, wu2)

    def partial(pair, w2, dtype, start=0):
        return down(pair[0], wd, pair[1], w2, dtype, start)

    h_own_near = hidden_pair(own_near)
    h_own_far = hidden_pair(own_far)
    h_near = hidden_pair(theirs_near)
    h_far = hidden_pair(theirs_far)
    far_a = pair_permute(partial(h_far, [wd2_a], BF16), n_dp, n_exp, False)
    far_b = pair_permute(partial(h_far, [wd2_b], BF16, half), n_dp, n_exp, False)
    own_far_a = partial(h_own_far, [wd2_a], F32)
    own_far_b = partial(h_own_far, [wd2_b], F32, half)
    near_part = pair_permute(partial(h_near, [wd2_a, wd2_b], BF16), n_dp, n_exp, False)
    own_near_part = partial(h_own_near, [wd2_a, wd2_b], F32)
    answer_a = add_and_split(own_far_a, far_a, len(far))
    answer_b = add_and_split(own_far_b, far_b, len(far))
    answer_near = add_and_split(own_near_part, near_part, len(near))
    if few(n_experts):
        back = expert_send(answer_near, near)
        back += expert_send(answer_a, far) + expert_send(answer_b, far)
    else:
        answer_far = [jnp.concatenate(pair, axis=1) for pair in zip(answer_a, answer_b)]
        back = [jnp.concatenate(expert_exchange(answer_near + answer_far), axis=0)]

    counts, _ = lax.optimization_barrier((counts, own_far[0, 0]))
    others = exchanged_counts(counts, answer_a[0][0, 0])
    corners = [(0, 0)]
    if few(n_experts):
        corners = [(k * most, 0) for k in near + far] + [(k * most, half) for k in far]
    return mix(ids, gate_units.T, capacity[None, :], others, here, back, corners, most)


def solution(mesh):
    return jax.shard_map(
        layer,
        mesh=mesh,
        in_specs=(
            P(AXES, None),
            P(AXES, None),
            P(AXES, None),
            P(),
            P("expert", None, "dp"),
            P("expert", None, "dp"),
            P("expert", None, "dp"),
        ),
        out_specs=P(AXES, None),
        check_vma=False,
    )
```

```python
import functools
import math

import jax
import jax.numpy as jnp
from jax import lax
from jax.experimental import pallas as pl
from jax.experimental.pallas import tpu as pltpu
from jax.sharding import PartitionSpec as P

BF16 = jnp.bfloat16
F32 = jnp.float32
AXES = ("dp", "expert")
VMEM_LIMIT = 8 << 20
BOTH_LAST = (((1,), (1,)), ((), ()))


def few(n):
    return n - 1 <= 16


def near_far(n):
    return list(range(n // 2)), list(range(n // 2, n))


def pair_permute(values, n_dp, n_exp, weights_side):
    pairs = []
    for d in range(n_dp):
        for e in range(n_exp):
            high = (e % 2 == 0) == weights_side
            partner = d ^ (n_dp // 2) if high else d ^ 1
            pairs.append((d * n_exp + e, partner * n_exp + e))
    return lax.ppermute(values, AXES, pairs)


def expert_exchange(blocks):
    n = lax.axis_size("expert")
    if not few(n):
        place = jnp.arange(n, dtype=jnp.int32) ^ lax.axis_index("expert")
        there = lax.all_to_all(jnp.stack(blocks)[place], "expert", 0, 0, tiled=True)[place]
        return [there[k] for k in range(n)]
    return expert_send(blocks, range(n))


def expert_send(blocks, places):
    n, out = lax.axis_size("expert"), []
    for k, block in zip(places, blocks):
        if k:
            block = lax.ppermute(block, "expert", [(i, i ^ k) for i in range(n)])
        out.append(block)
    return out


def exchanged_counts(counts, late):
    n = lax.axis_size("dp") * lax.axis_size("expert")
    total, others = counts, []
    step = 1
    while step < n:
        if step == lax.axis_size("expert"):
            total, _ = lax.optimization_barrier((total, late))
        others.append(lax.ppermute(total, AXES, [(i, i ^ step) for i in range(n)]))
        total = total + others[-1]
        step *= 2
    return others


def dot(a, b):
    return jnp.dot(a, b, preferred_element_type=F32)


def kernel_call(body, shapes, operands, flops):
    spec = pl.BlockSpec(memory_space=pltpu.VMEM)
    single = not isinstance(shapes, (list, tuple))
    moved = sum(x.size * x.dtype.itemsize for x in operands)
    return pl.pallas_call(
        body,
        out_shape=shapes if single else tuple(shapes),
        in_specs=[spec] * len(operands),
        out_specs=spec if single else tuple([spec] * len(shapes)),
        compiler_params=pltpu.CompilerParams(vmem_limit_bytes=VMEM_LIMIT),
        cost_estimate=pl.CostEstimate(flops=flops, bytes_accessed=moved, transcendentals=0),
    )(*operands)


def join(blocks):
    if len(blocks) > 16:
        return jnp.concatenate(blocks, axis=0)
    rows, width = blocks[0].shape

    def body(*refs):
        for i, ref in enumerate(refs[:-1]):
            refs[-1][i * rows : (i + 1) * rows, :] = ref[...]

    shape = jax.ShapeDtypeStruct((rows * len(blocks), width), blocks[0].dtype)
    return kernel_call(body, shape, blocks, 0)


def hidden_of(rows, gate_t, up_t):
    def body(rows_ref, gate_ref, up_ref, out_ref):
        gate = lax.dot_general(rows_ref[...], gate_ref[...], BOTH_LAST, preferred_element_type=F32)
        up = lax.dot_general(rows_ref[...], up_ref[...], BOTH_LAST, preferred_element_type=F32)
        out_ref[...] = (gate / (1.0 + jnp.exp(-gate)) * up).astype(BF16)

    units = gate_t.shape[0]
    shape = jax.ShapeDtypeStruct((rows.shape[0], units), BF16)
    return kernel_call(body, shape, (rows, gate_t, up_t), 4 * rows.size * units)


def down(hidden, down_t, hidden2, down2_t, dtype, start=0, parts=1):
    width = sum(piece.shape[1] for piece in down2_t)
    step = math.gcd(*(piece.shape[1] for piece in down2_t), 512)

    def body(h_ref, w_ref, h2_ref, *refs):
        at = 0
        for ref in refs[:-parts]:
            for here in range(0, ref.shape[1], step):
                columns = slice(start + at, start + at + step)
                part = dot(h_ref[...], w_ref[:, columns]) + dot(h2_ref[...], ref[:, here : here + step])
                for i, out_ref in enumerate(refs[-parts:]):
                    out_ref[:, at : at + step] = part[i * rows : (i + 1) * rows, :].astype(dtype)
                at += step

    rows = hidden.shape[0] // parts
    shape = jax.ShapeDtypeStruct((rows, width), dtype)
    shapes = shape if parts == 1 else [shape] * parts
    return kernel_call(body, shapes, (hidden, down_t, hidden2, *down2_t), 4 * hidden.size * width)


def add_and_split(own, returned, count):
    rows, width = own.shape[0] // count, own.shape[1]
    if count > 16:
        total = (own + returned.astype(F32)).astype(BF16).reshape(count, rows, width)
        return [total[k] for k in range(count)]

    def body(own_ref, returned_ref, *out_refs):
        for k, ref in enumerate(out_refs):
            part = slice(k * rows, (k + 1) * rows)
            ref[...] = (own_ref[part, :] + returned_ref[part, :].astype(F32)).astype(BF16)

    shapes = [jax.ShapeDtypeStruct((rows, width), BF16)] * count
    return list(kernel_call(body, shapes, (own, returned), own.size))


def named_places(ids, me, n):
    rows = ids.shape[1]
    place = lax.broadcasted_iota(jnp.int32, (n, rows), 0)
    named = [(ids[k : k + 1, :] ^ me) == place for k in range(ids.shape[0])]
    once = functools.reduce(jnp.logical_or, named)
    first = lax.broadcasted_iota(jnp.int32, (rows, rows), 0)
    second = lax.broadcasted_iota(jnp.int32, (rows, rows), 1)
    earlier = dot(ones_at(once), ones_at(first < second))
    return named, once, earlier


def ones_at(mask):
    return jnp.where(mask, 1.0, 0.0).astype(BF16)


def dispatch(tokens, ids, here, n, most):
    tok_rows, width = tokens.shape

    def body(tokens_ref, ids_ref, here_ref, counts_ref, *out_refs):
        me = here_ref[0, 0] % n
        _, once, earlier = named_places(ids_ref[...], me, n)
        _, absolute, _ = named_places(ids_ref[...], 0, n)
        ones = jnp.ones((1, tok_rows), BF16)
        counts = lax.dot_general(ones, ones_at(absolute), BOTH_LAST, preferred_element_type=F32)
        counts_ref[...] = counts.astype(jnp.int32)
        slot = jnp.where(once, earlier, -1.0)
        row = lax.broadcasted_iota(jnp.int32, (most, tok_rows), 0).astype(F32)
        for k in range(n):
            picked = dot(ones_at(row == slot[k : k + 1, :]), tokens_ref[...]).astype(BF16)
            if few(n):
                out_refs[k][...] = picked
            else:
                out_refs[0][k] = picked

    shapes = [jax.ShapeDtypeStruct((1, n), jnp.int32)]
    if few(n):
        shapes += [jax.ShapeDtypeStruct((most, width), BF16)] * n
    else:
        shapes += [jax.ShapeDtypeStruct((n, most, width), BF16)]
    memory = [pltpu.VMEM, pltpu.VMEM, pltpu.SMEM]
    call = pl.pallas_call(
        body,
        out_shape=tuple(shapes),
        in_specs=[pl.BlockSpec(memory_space=m) for m in memory],
        out_specs=tuple(pl.BlockSpec(memory_space=pltpu.VMEM) for _ in shapes),
        compiler_params=pltpu.CompilerParams(vmem_limit_bytes=VMEM_LIMIT),
        name="dispatch",
    )
    counts, *blocks = call(tokens, ids, here)
    return [blocks[0][k] for k in range(n)] if len(blocks) < n else blocks, counts


def mix_weights(ids, units, capacity, others, here, most):
    n, tok_rows = capacity.shape[1], ids.shape[1]

    def body(here_ref, ids_ref, units_ref, capacity_ref, *refs):
        out_ref = refs[-1]
        me = here_ref[0, 0]
        room = capacity_ref[...]
        for i, ref in enumerate(refs[:-1]):
            room = room - ref[...] * ((me >> i) & 1)
        place = lax.broadcasted_iota(jnp.int32, (n, n), 0)
        expert = lax.broadcasted_iota(jnp.int32, (n, n), 1)
        room = jnp.sum(jnp.where(place ^ (me % n) == expert, room, 0).astype(F32), axis=1, keepdims=True)
        named, once, earlier = named_places(ids_ref[...], me % n, n)
        unit = sum(jnp.where(named[k], units_ref[k : k + 1, :], 0) for k in range(len(named)))
        unit = jnp.where(earlier < room, unit, 0)
        high = ((unit >> 3) << 3).astype(F32) * (1.0 / 1024.0)
        low = (unit & 7).astype(F32) * (1.0 / 1024.0)
        slot = jnp.where(once, earlier, -1.0)
        row = lax.broadcasted_iota(jnp.int32, (most, tok_rows), 0).astype(F32)
        for i, values in enumerate((high, low)):
            parts = [jnp.where(row == slot[k : k + 1, :], values[k : k + 1, :], 0.0) for k in range(n)]
            spread = jnp.concatenate(parts, axis=0)
            out_ref[i * tok_rows : (i + 1) * tok_rows, :] = spread.T.astype(BF16)

    operands = (here, ids, units, capacity, *others)
    memory = [pltpu.SMEM] + [pltpu.VMEM] * (len(operands) - 1)
    return pl.pallas_call(
        body,
        out_shape=jax.ShapeDtypeStruct((2 * tok_rows, n * most), BF16),
        in_specs=[pl.BlockSpec(memory_space=m) for m in memory],
        out_specs=pl.BlockSpec(memory_space=pltpu.VMEM),
        compiler_params=pltpu.CompilerParams(vmem_limit_bytes=VMEM_LIMIT),
        name="mix_weights",
    )(*operands)


def mix(weights, back, corners):
    tok_rows, choices = weights.shape[0] // 2, weights.shape[1]
    width = sum(b.size for b in back) // choices

    def body(weights_ref, *refs):
        out_ref, joined = refs[-2:]
        for at, ref in zip(corners, refs[:-2]):
            joined[at[0] : at[0] + ref.shape[0], at[1] : at[1] + ref.shape[1]] = ref[...]
        step = math.gcd(width, 256)
        for column in range(0, width, step):
            here = slice(column, column + step)
            both = dot(weights_ref[...], joined[:, here])
            out_ref[:, here] = (both[:tok_rows, :] + both[tok_rows:, :]).astype(BF16)

    return pl.pallas_call(
        body,
        out_shape=jax.ShapeDtypeStruct((tok_rows, width), BF16),
        in_specs=[pl.BlockSpec(memory_space=pltpu.VMEM)] * (1 + len(back)),
        out_specs=pl.BlockSpec(memory_space=pltpu.VMEM),
        scratch_shapes=[pltpu.VMEM((choices, width), BF16)],
        compiler_params=pltpu.CompilerParams(vmem_limit_bytes=VMEM_LIMIT),
        name="mix",
    )(weights, *back)


def layer(tokens, expert_ids, gate_units, capacity, w_gate, w_up, w_down):
    n_dp, n_exp = lax.axis_size("dp"), lax.axis_size("expert")
    tok_rows, width = tokens.shape
    n_experts = capacity.shape[0]
    most = max(2, 5 * tok_rows // (2 * n_experts))
    here = jnp.full((1, 1), lax.axis_index(AXES), jnp.int32)
    near, far = near_far(n_experts)
    wg, wu, wd = w_gate[0].T, w_up[0].T, w_down[0].T
    here, wg, wu, wd = lax.optimization_barrier((here, wg, wu, wd))
    wg2 = pair_permute(wg, n_dp, n_exp, True)
    wu2 = pair_permute(wu, n_dp, n_exp, True)
    half = width * 3 // 8
    wd2_a = pair_permute(wd[:, :half], n_dp, n_exp, True)
    wd2_b = pair_permute(wd[:, half:], n_dp, n_exp, True)

    ids = expert_ids.T
    blocks, counts = dispatch(tokens, ids, here, n_experts, most)
    arrived = expert_exchange(blocks)
    own_near = join([arrived[k] for k in near])
    theirs_near = pair_permute(own_near, n_dp, n_exp, False)
    own_far = join([arrived[k] for k in far])
    theirs_far = pair_permute(own_far, n_dp, n_exp, False)

    def hidden_pair(rows):
        return hidden_of(rows, wg, wu), hidden_of(rows, wg2, wu2)

    def partial(pair, w2, dtype, start=0, parts=1):
        return down(pair[0], wd, pair[1], w2, dtype, start, parts)

    h_own_near = hidden_pair(own_near)
    h_own_far = hidden_pair(own_far)
    h_near = hidden_pair(theirs_near)
    h_far = hidden_pair(theirs_far)
    far_a = pair_permute(partial(h_far, [wd2_a], BF16), n_dp, n_exp, False)
    far_b = pair_permute(partial(h_far, [wd2_b], BF16, half), n_dp, n_exp, False)
    own_far_a = partial(h_own_far, [wd2_a], F32)
    own_far_b = partial(h_own_far, [wd2_b], F32, half)
    near_part = partial(h_near, [wd2_a, wd2_b], BF16, parts=2)
    near_part = [pair_permute(p, n_dp, n_exp, False) for p in near_part]
    own_near_part = partial(h_own_near, [wd2_a, wd2_b], F32, parts=2)
    answer_a = add_and_split(own_far_a, far_a, len(far))
    answer_b = add_and_split(own_far_b, far_b, len(far))
    answer_near = add_and_split(own_near_part[0], near_part[0], len(near) // 2)
    answer_near += add_and_split(own_near_part[1], near_part[1], len(near) // 2)
    if few(n_experts):
        back = expert_send(answer_near, near)
        back += expert_send(answer_a, far) + expert_send(answer_b, far)
    else:
        answer_far = [jnp.concatenate(pair, axis=1) for pair in zip(answer_a, answer_b)]
        back = [jnp.concatenate(expert_exchange(answer_near + answer_far), axis=0)]

    counts, _ = lax.optimization_barrier((counts, own_far[0, 0]))
    others = exchanged_counts(counts, answer_a[0][0, 0])
    corners = [(0, 0)]
    if few(n_experts):
        corners = [(k * most, 0) for k in near + far] + [(k * most, half) for k in far]
    weights = mix_weights(ids, gate_units.T, capacity[None, :], others, here, most)
    return mix(weights, back, corners)


def solution(mesh):
    return jax.shard_map(
        layer,
        mesh=mesh,
        in_specs=(
            P(AXES, None),
            P(AXES, None),
            P(AXES, None),
            P(),
            P("expert", None, "dp"),
            P("expert", None, "dp"),
            P("expert", None, "dp"),
        ),
        out_specs=P(AXES, None),
        check_vma=False,
    )
```
